32 devices in a mesh: row: 4 (over z), col: 8 (over y, x, core).
Axes of the slice: x: 2, y: 2, z: 4, core: 2. Of those that a mesh axis runs over, the one named last changes fastest.
Arguments:
- tri_panels: float32 [8192, 4096], P('row', 'col'), may hold values from -1 to 2, as said below
- rhs_rows: float32 [8192, 1024], P(('row', 'col')), may hold values from -6 to 6
Outputs:
- rhs_grid: float32 [8192, 1024], P('row', 'col')
The draws below stay inside these ranges and needn't reach their ends.
Inputs may be any that keep to these rules, and one draw needn't show every extreme that they name: `tri_panels`: in L's row order the entries above the diagonal are zero and the diagonal entries are positive.
All inputs are finite; a program needn't handle non-finite values.
Results may differ from the reference program's by a relative error of at most 0.00011.
Values sent between devices are 32-bit elements; how exact they have to be, the bound alone decides.
A program may use at most 256 MiB of HBM per device.

```python
import math
import jax
import jax.numpy as jnp
from jax import lax

N = 8192
NB = 512
NRHS = 1024
K = 4096
N_ROW = 4
N_COL = 8


def draw_tri_panels(key, part):
    key_offdiag = jax.random.fold_in(key, 11)
    key_diagonal = jax.random.fold_in(key, 23)
    bound_value = 2.7 / math.sqrt(N)
    off_diagonal = jax.random.uniform(key_offdiag, (N, K), jnp.float32, -bound_value, bound_value)
    diagonal_values = jnp.exp(jax.random.uniform(key_diagonal, (N,), jnp.float32, 0.0, math.log(2.0)))
    row_index = jnp.arange(N, dtype=jnp.int32)[:, None]
    col_index = jnp.arange(K, dtype=jnp.int32)[None, :]
    matrix_lower = jnp.where(row_index > col_index, off_diagonal, jnp.float32(0.0))
    matrix_lower = jnp.where(row_index == col_index, diagonal_values[:, None], matrix_lower)
    block_count = N // (N_ROW * NB)
    return matrix_lower.reshape(block_count, N_ROW, NB, K).transpose(1, 0, 2, 3).reshape(N, K)


def level_of(rng, shape, cuts, least, high):
    def one(axis_at, parts):
        steps = jax.random.uniform(jax.random.fold_in(jax.random.fold_in(rng, 6), axis_at), (parts,), jnp.float32, least / len(cuts), high / len(cuts))
        return jnp.repeat(jnp.exp(steps), shape[axis_at] // parts).reshape((-1,) + (1,) * (len(shape) - axis_at - 1))

    gain = one(*cuts[0])
    for cut in cuts[1:]:
        gain = gain * one(*cut)
    return gain


def normal_values(key, extent, deviation, most, pieces=(), kind=jnp.bfloat16):
    factor_of = level_of(key, extent, pieces, -0.22, 0.18) if pieces else 1.0
    drawn = jax.random.normal(key, extent, jnp.float32) * deviation * factor_of
    return jnp.minimum(jnp.maximum(drawn, -most), most).astype(kind)


def setup_inputs(seed: int = 0) -> dict:
    splits = jax.random.split(jax.random.key(seed), 3)
    return {
        "tri_panels": draw_tri_panels(jax.random.fold_in(splits[2], 71), 0),
        "rhs_rows": normal_values(splits[1], (N, NRHS), 1.0, 6.0, ((0, 32),), jnp.float32),
    }


def reference(tri_panels, rhs_rows):
    block_count = N // (N_ROW * NB)
    sub_rows = NB // N_COL
    lower_full = tri_panels.reshape(N_ROW, block_count, NB, K).transpose(1, 0, 2, 3).reshape(N, K)
    right_side = rhs_rows.reshape(N_ROW, N_COL, block_count, sub_rows, NRHS).transpose(2, 0, 1, 3, 4).reshape(N, NRHS)
    for step_index in range(N_COL):
        top_row = step_index * NB
        bottom = top_row + NB
        solution = jax.scipy.linalg.solve_triangular(lower_full[top_row:bottom, top_row:bottom], right_side[top_row:bottom], lower=True)
        below_rows = right_side[bottom:] - jnp.dot(lower_full[bottom:, top_row:bottom].astype(jnp.float32), solution.astype(jnp.float32), precision=lax.Precision.HIGHEST, preferred_element_type=jnp.float32)
        right_side = jnp.concatenate([right_side[:top_row], solution, below_rows], 0)
    return right_side.reshape(block_count, N_ROW, NB, NRHS).transpose(1, 0, 2, 3).reshape(N, NRHS)
```

```python
import functools

import jax
import jax.numpy as jnp
from jax import lax
from jax.experimental import pallas as pl
from jax.experimental.pallas import tpu as pltpu
from jax.sharding import PartitionSpec as P

HIGHEST = lax.Precision.HIGHEST


def dot(a, b):
    return jnp.dot(a, b, precision=HIGHEST, preferred_element_type=jnp.float32)


def steps_kernel(
    row_count, col_count, panels_ref, inverses_ref, state_in_ref, solved_ref, state_ref,
    panels, inverses, panel_sem, inverse_sem, state_sem, send_sem, recv_sem,
):
    row = lax.axis_index("row")
    slots, size, _ = state_ref.shape

    def panel_copy(k):
        return pltpu.make_async_copy(
            panels_ref.at[:, pl.ds(pl.multiple_of(k * size, size), size)],
            panels.at[k],
            panel_sem.at[k],
        )

    def inverse_copy(s):
        block = jnp.minimum(s * row_count + row, col_count - 1)
        return pltpu.make_async_copy(
            inverses_ref.at[:, pl.ds(pl.multiple_of(block * size, size), size)],
            inverses.at[s],
            inverse_sem.at[s],
        )

    state_copy = pltpu.make_async_copy(state_in_ref, state_ref, state_sem)
    state_copy.start()
    for s in range(slots):
        inverse_copy(s).start()
    for k in range(col_count):
        panel_copy(k).start()

    barrier = pltpu.get_barrier_semaphore()
    for shift in range(1, row_count):
        pl.semaphore_signal(
            barrier, inc=1, device_id={"row": lax.rem(row + shift, row_count)},
            device_id_type=pl.DeviceIdType.MESH,
        )
    pl.semaphore_wait(barrier, row_count - 1)
    state_copy.wait()
    for s in range(slots):
        inverse_copy(s).wait()

    def remote(k, shift):
        return pltpu.make_async_remote_copy(
            src_ref=solved_ref.at[k],
            dst_ref=solved_ref.at[k],
            send_sem=send_sem.at[shift - 1],
            recv_sem=recv_sem.at[k],
            device_id={"row": lax.rem(row + shift, row_count)},
            device_id_type=pl.DeviceIdType.MESH,
        )

    def update(k, s):
        part = panels[k, pl.ds(pl.multiple_of(s * size, size), size), :]
        state_ref[s] = state_ref[s] - dot(part, solved_ref[k])

    def update_all(k, skipped):
        def one(s, carry):
            @pl.when((s * row_count + row > k) & (s != skipped))
            def _():
                update(k, s)

            return carry

        lax.fori_loop(0, slots, one, 0)

    def step(k, carry):
        owner = lax.rem(k, row_count)
        slot = lax.div(k, row_count)

        @pl.when(row == owner)
        def _():
            @pl.when(k > 0)
            def _():
                update(k - 1, slot)

            solved = dot(inverses[slot], state_ref[slot])
            solved_ref[k] = solved
            for shift in range(1, row_count):
                remote(k, shift).start()
            state_ref[slot] = solved

            @pl.when(k > 0)
            def _():
                update_all(k - 1, slot)

        @pl.when(row != owner)
        def _():
            remote(k, 1).wait_recv()

        panel_copy(k).wait()

        @pl.when((row != lax.rem(k + 1, row_count)) | (k == col_count - 1))
        def _():
            update_all(k, -1)

        @pl.when(row == owner)
        def _():
            for shift in range(1, row_count):
                remote(k, shift).wait_send()

        return carry

    lax.fori_loop(0, col_count, step, 0)


def run_steps(panels, inverses, state):
    row_count = lax.axis_size("row")
    slots, size, width = state.shape
    col_count = panels.shape[1] // size
    anywhere = pl.BlockSpec(memory_space=pl.ANY)
    inside = pl.BlockSpec(memory_space=pltpu.VMEM)
    return pl.pallas_call(
        functools.partial(steps_kernel, row_count, col_count),
        out_shape=(
            jax.ShapeDtypeStruct((col_count, size, width), jnp.float32),
            jax.ShapeDtypeStruct((slots, size, width), jnp.float32),
        ),
        in_specs=[anywhere, anywhere, anywhere],
        out_specs=(inside, inside),
        scratch_shapes=[
            pltpu.VMEM((col_count, slots * size, size), jnp.float32),
            pltpu.VMEM((slots, size, size), jnp.float32),
            pltpu.SemaphoreType.DMA((col_count,)),
            pltpu.SemaphoreType.DMA((slots,)),
            pltpu.SemaphoreType.DMA,
            pltpu.SemaphoreType.DMA((row_count - 1,)),
            pltpu.SemaphoreType.DMA((col_count,)),
        ],
        compiler_params=pltpu.CompilerParams(
            collective_id=0, has_side_effects=True, vmem_limit_bytes=48 * 1024 * 1024
        ),
        cost_estimate=pl.CostEstimate(
            flops=60 * size * size * width * 2 * 6, bytes_accessed=24 << 20, transcendentals=0
        ),
    )(panels, inverses, state)


def on_device(tri_panels, rhs_rows):
    row_count = lax.axis_size("row")
    col_count = lax.axis_size("col")
    row_position = lax.axis_index("row")
    col_position = lax.axis_index("col")
    local_rows, size = tri_panels.shape
    blocks = local_rows // size
    sub_rows = size // col_count
    slots = min((col_count + row_count - 1) // row_count, blocks)
    parted = rhs_rows.reshape(blocks, sub_rows, rhs_rows.shape[1])
    state_rhs = lax.all_to_all(parted, "col", split_axis=2, concat_axis=1, tiled=True)
    identity_block = jnp.eye(size, dtype=jnp.float32)
    own_pieces = tri_panels.reshape(blocks, size, size)
    own_diag = lax.dynamic_index_in_dim(own_pieces, col_position // row_count, 0, keepdims=False)
    own_diag = jnp.where(col_position % row_count == row_position, own_diag, identity_block)
    own_inverse = jax.scipy.linalg.solve_triangular(own_diag, identity_block, lower=True)
    top = lax.all_gather(tri_panels[: slots * size], "col", axis=1, tiled=True)
    inverses = lax.all_gather(own_inverse, "col", axis=1, tiled=True)
    solved, state_top = run_steps(top, inverses, state_rhs[:slots])
    width = state_rhs.shape[2]
    state_top = state_top.reshape(slots * size, width)
    if slots == blocks:
        return state_top
    below = lax.all_gather(tri_panels[slots * size :], "col", axis=1, tiled=True)
    product = dot(below, solved.reshape(col_count * size, width))
    state_below = state_rhs[slots:].reshape((blocks - slots) * size, width) - product
    return jnp.concatenate([state_top, state_below], 0)


def solution(mesh):
    return jax.shard_map(
        on_device,
        mesh=mesh,
        in_specs=(P("row", "col"), P(("row", "col"), None)),
        out_specs=P("row", "col"),
        check_vma=False,
    )
```

```python
import functools

import jax
import jax.numpy as jnp
from jax import lax
from jax.experimental import pallas as pl
from jax.experimental.pallas import tpu as pltpu
from jax.sharding import PartitionSpec as P

HIGHEST = lax.Precision.HIGHEST


def dot(a, b):
    return jnp.dot(a, b, precision=HIGHEST, preferred_element_type=jnp.float32)


def steps_kernel(
    row_count, col_count, panels_ref, inverses_ref, state_in_ref, solved_ref, state_ref,
    panels, inverses, panel_sem, inverse_sem, state_sem, send_sem, recv_sem,
):
    row = lax.axis_index("row")
    slots, size, _ = state_ref.shape

    def panel_copy(k):
        return pltpu.make_async_copy(
            panels_ref.at[:, pl.ds(pl.multiple_of(k * size, size), size)],
            panels.at[k],
            panel_sem.at[k],
        )

    def inverse_copy(s):
        block = jnp.minimum(s * row_count + row, col_count - 1)
        return pltpu.make_async_copy(
            inverses_ref.at[:, pl.ds(pl.multiple_of(block * size, size), size)],
            inverses.at[s],
            inverse_sem.at[s],
        )

    state_copy = pltpu.make_async_copy(state_in_ref, state_ref, state_sem)
    state_copy.start()
    for s in range(slots):
        inverse_copy(s).start()
    for k in range(col_count):
        panel_copy(k).start()

    barrier = pltpu.get_barrier_semaphore()
    for shift in range(1, row_count):
        pl.semaphore_signal(
            barrier, inc=1, device_id={"row": lax.rem(row + shift, row_count)},
            device_id_type=pl.DeviceIdType.MESH,
        )
    pl.semaphore_wait(barrier, row_count - 1)
    state_copy.wait()
    for s in range(slots):
        inverse_copy(s).wait()

    def remote(k, shift):
        return pltpu.make_async_remote_copy(
            src_ref=solved_ref.at[k],
            dst_ref=solved_ref.at[k],
            send_sem=send_sem.at[shift - 1],
            recv_sem=recv_sem.at[k],
            device_id={"row": lax.rem(row + shift, row_count)},
            device_id_type=pl.DeviceIdType.MESH,
        )

    def update(k, s):
        part = panels[k, pl.ds(pl.multiple_of(s * size, size), size), :]
        state_ref[s] = state_ref[s] - dot(part, solved_ref[k])

    def update_all(k, skipped):
        def one(s, carry):
            @pl.when((s * row_count + row > k) & (s != skipped))
            def _():
                update(k, s)

            return carry

        lax.fori_loop(0, slots, one, 0)

    def step(k, carry):
        owner = lax.rem(k, row_count)
        slot = lax.div(k, row_count)

        @pl.when(row == owner)
        def _():
            @pl.when(k > 0)
            def _():
                update(k - 1, slot)

            solved = dot(inverses[slot], state_ref[slot])
            solved_ref[k] = solved
            for shift in range(1, row_count):
                remote(k, shift).start()
            state_ref[slot] = solved

            @pl.when(k > 0)
            def _():
                update_all(k - 1, slot)

        @pl.when(row != owner)
        def _():
            remote(k, 1).wait_recv()

        panel_copy(k).wait()

        @pl.when((row != lax.rem(k + 1, row_count)) | (k == col_count - 1))
        def _():
            update_all(k, -1)

        @pl.when(row == owner)
        def _():
            for shift in range(1, row_count):
                remote(k, shift).wait_send()

        return carry

    lax.fori_loop(0, col_count, step, 0)


def run_steps(panels, inverses, state):
    row_count = lax.axis_size("row")
    slots, size, width = state.shape
    col_count = panels.shape[1] // size
    anywhere = pl.BlockSpec(memory_space=pl.ANY)
    inside = pl.BlockSpec(memory_space=pltpu.VMEM)
    return pl.pallas_call(
        functools.partial(steps_kernel, row_count, col_count),
        out_shape=(
            jax.ShapeDtypeStruct((col_count, size, width), jnp.float32),
            jax.ShapeDtypeStruct((slots, size, width), jnp.float32),
        ),
        in_specs=[anywhere, anywhere, anywhere],
        out_specs=(inside, inside),
        scratch_shapes=[
            pltpu.VMEM((col_count, slots * size, size), jnp.float32),
            pltpu.VMEM((slots, size, size), jnp.float32),
            pltpu.SemaphoreType.DMA((col_count,)),
            pltpu.SemaphoreType.DMA((slots,)),
            pltpu.SemaphoreType.DMA,
            pltpu.SemaphoreType.DMA((row_count - 1,)),
            pltpu.SemaphoreType.DMA((col_count,)),
        ],
        compiler_params=pltpu.CompilerParams(
            collective_id=0, has_side_effects=True, vmem_limit_bytes=48 * 1024 * 1024
        ),
        cost_estimate=pl.CostEstimate(
            flops=240 * size * size * width * 2 * 6, bytes_accessed=24 << 20, transcendentals=0
        ),
    )(panels, inverses, state)


def on_device(tri_panels, rhs_rows):
    row_count = lax.axis_size("row")
    col_count = lax.axis_size("col")
    row_position = lax.axis_index("row")
    col_position = lax.axis_index("col")
    local_rows, size = tri_panels.shape
    blocks = local_rows // size
    sub_rows = size // col_count
    slots = min((col_count + row_count - 1) // row_count, blocks)
    parted = rhs_rows.reshape(blocks, sub_rows, rhs_rows.shape[1])
    state_rhs = lax.all_to_all(parted, "col", split_axis=2, concat_axis=1, tiled=True)
    identity_block = jnp.eye(size, dtype=jnp.float32)
    own_pieces = tri_panels.reshape(blocks, size, size)
    own_diag = lax.dynamic_index_in_dim(own_pieces, col_position // row_count, 0, keepdims=False)
    own_diag = jnp.where(col_position % row_count == row_position, own_diag, identity_block)
    own_inverse = jax.scipy.linalg.solve_triangular(own_diag, identity_block, lower=True)
    top = lax.all_gather(tri_panels[: slots * size], "col", axis=1, tiled=True)
    top, own_inverse = lax.optimization_barrier((top, own_inverse))
    inverses = lax.all_gather(own_inverse, "col", axis=1, tiled=True)
    inverses, tri_panels = lax.optimization_barrier((inverses, tri_panels))
    solved, state_top = run_steps(top, inverses, state_rhs[:slots])
    width = state_rhs.shape[2]
    state_top = state_top.reshape(slots * size, width)
    if slots == blocks:
        return state_top
    below = lax.all_gather(tri_panels[slots * size :], "col", axis=1, tiled=True)
    product = dot(below, solved.reshape(col_count * size, width))
    state_below = state_rhs[slots:].reshape((blocks - slots) * size, width) - product
    return jnp.concatenate([state_top, state_below], 0)


def solution(mesh):
    return jax.shard_map(
        on_device,
        mesh=mesh,
        in_specs=(P("row", "col"), P(("row", "col"), None)),
        out_specs=P("row", "col"),
        check_vma=False,
    )
```
